16 devices in a mesh: dp: 4 (over z, y), sp: 4 (over x, core).
Axes of the slice: x: 2, y: 2, z: 2, core: 2. Of those that a mesh axis runs over, the one named last changes fastest.
Arguments:
- images: bfloat16 [64, 16, 512, 256], P('dp', 'sp'), parts along dimension 0
- w_a: bfloat16 [4, 3, 3, 256, 256], replicated
- bn_a: float32 [4, 2, 256], replicated
- w_down: bfloat16 [3, 3, 256, 2048], replicated
- bn_down: float32 [2, 2048], replicated
- w_in: bfloat16 [2, 2048, 512], replicated
- bn_in: float32 [2, 2, 512], replicated
- w_mid: bfloat16 [2, 3, 3, 512, 512], replicated
- bn_mid: float32 [2, 2, 512], replicated
- w_out: bfloat16 [2, 512, 2048], replicated
- bn_out: float32 [2, 2, 2048], replicated
Outputs:
- output: bfloat16 [64, 8, 256, 2048], P('dp', 'sp'), parts along dimension 0
There are 4 independent parts. The reference program is written for one: setup_inputs(seed, part) draws one part's arguments, and reference() takes and returns one part's arrays. A program takes and returns all parts, laid end to end along the dimension named above; an argument that names none is the same for every part.
All inputs are finite; a program needn't handle non-finite values.
Results may differ from the reference program's by a relative error of at most 0.02.
Values are sent between devices in bfloat16 or wider.
A program may use at most 1 GiB of HBM per device.

```python
import jax
import jax.numpy as jnp
from jax import lax

IMAGES = 16
ROWS_DEV = 4
IMG_WIDTH = 512
LAYERS_A = 4
BLOCKS_B = 2
CHAN_A = 256
CHAN_MID = 512
CHAN_B = 2048
GROUP_SIZE = 4
NORM_EPS = 1e-5
CONV_DIMS = ("NHWC", "HWIO", "NHWC")


def conv_weight(draw_key, full_shape, fan_in):
    return (jax.random.normal(draw_key, full_shape, jnp.float32) * fan_in ** -0.5).astype(jnp.bfloat16)


def norm_params(draw_key, lead_dims, chan_count):
    key_gain, key_shift = jax.random.split(draw_key)
    norm_gain = jax.random.uniform(key_gain, lead_dims + (chan_count,), jnp.float32, 0.6, 1.4)
    norm_shift = 0.4 * jax.random.normal(key_shift, lead_dims + (chan_count,), jnp.float32)
    return jnp.stack([norm_gain, norm_shift], axis=-2)


def setup_inputs(seed: int = 0, part: int = 0) -> dict:
    base_key = jax.random.key(seed)
    part_key = jax.random.fold_in(base_key, part)
    key_noise, key_amp, key_phase = jax.random.split(part_key, 3)
    weight_keys = jax.random.split(base_key, 10)
    height = GROUP_SIZE * ROWS_DEV
    row_pos = (jnp.arange(height, dtype=jnp.float32) + 0.5) / height
    band_amp = 1.5 * jax.random.normal(key_amp, (CHAN_A,), jnp.float32)
    band_phase = 6.2832 * jax.random.uniform(key_phase, (CHAN_A,), jnp.float32)
    row_band = band_amp * (1.0 - 2.0 * row_pos)[:, None] + jnp.sin(12.566 * row_pos[:, None] + band_phase)
    pixel_noise = jax.random.normal(key_noise, (IMAGES, height, IMG_WIDTH, CHAN_A), jnp.float32)
    return {
        "images": (pixel_noise + row_band[None, :, None, :]).astype(jnp.bfloat16),
        "w_a": conv_weight(weight_keys[0], (LAYERS_A, 3, 3, CHAN_A, CHAN_A), 9 * CHAN_A),
        "bn_a": norm_params(weight_keys[1], (LAYERS_A,), CHAN_A),
        "w_down": conv_weight(weight_keys[2], (3, 3, CHAN_A, CHAN_B), 9 * CHAN_A),
        "bn_down": norm_params(weight_keys[3], (), CHAN_B),
        "w_in": conv_weight(weight_keys[4], (BLOCKS_B, CHAN_B, CHAN_MID), CHAN_B),
        "bn_in": norm_params(weight_keys[5], (BLOCKS_B,), CHAN_MID),
        "w_mid": conv_weight(weight_keys[6], (BLOCKS_B, 3, 3, CHAN_MID, CHAN_MID), 9 * CHAN_MID),
        "bn_mid": norm_params(weight_keys[7], (BLOCKS_B,), CHAN_MID),
        "w_out": conv_weight(weight_keys[8], (BLOCKS_B, CHAN_MID, CHAN_B), CHAN_MID),
        "bn_out": norm_params(weight_keys[9], (BLOCKS_B,), CHAN_B),
    }


def conv_full(hidden, weight, stride):
    return lax.conv_general_dilated(hidden.astype(jnp.float32), weight.astype(jnp.float32), (stride, stride), "SAME", dimension_numbers=CONV_DIMS)


def conv_point(hidden, weight):
    return jnp.einsum("bhwc,cd->bhwd", hidden.astype(jnp.float32), weight.astype(jnp.float32))


def batch_norm(pre_act, params):
    chan_mean = jnp.mean(pre_act, axis=(0, 1, 2))
    chan_var = jnp.mean(pre_act * pre_act, axis=(0, 1, 2)) - chan_mean * chan_mean
    chan_scale = params[0] * lax.rsqrt(chan_var + NORM_EPS)
    return (pre_act - chan_mean) * chan_scale + params[1]


def norm_relu(pre_act, params):
    return jax.nn.relu(batch_norm(pre_act, params)).astype(jnp.bfloat16)


def reference(images, w_a, bn_a, w_down, bn_down, w_in, bn_in, w_mid, bn_mid, w_out, bn_out):
    def stage_a(hidden, layer_args):
        return norm_relu(conv_full(hidden, layer_args[0], 1), layer_args[1]), None

    def bottleneck(hidden, block_args):
        w_first, bn_first, w_three, bn_three, w_last, bn_last = block_args
        branch = norm_relu(conv_point(hidden, w_first), bn_first)
        branch = norm_relu(conv_full(branch, w_three, 1), bn_three)
        summed = batch_norm(conv_point(branch, w_last), bn_last) + hidden.astype(jnp.float32)
        return jax.nn.relu(summed).astype(jnp.bfloat16), None

    hidden, _ = lax.scan(stage_a, images, (w_a, bn_a))
    hidden = norm_relu(conv_full(hidden, w_down, 2), bn_down)
    hidden, _ = lax.scan(bottleneck, hidden, (w_in, bn_in, w_mid, bn_mid, w_out, bn_out))
    return hidden
```

```python
import functools

import jax
import jax.numpy as jnp
from jax import lax
from jax.experimental import pallas as pl
from jax.experimental.pallas import tpu as pltpu
from jax.sharding import PartitionSpec as P

NORM_EPS = 1e-5
BF, F32 = jnp.bfloat16, jnp.float32
TILE = 256
LEAD = 3
VMEM = 64000 * 1024


def coefficients(tot_ref, bn_ref, count):
    mean = tot_ref[0:1, :] / count
    var = tot_ref[1:2, :] / count - mean * mean
    return mean, bn_ref[0:1, :] * lax.rsqrt(var + NORM_EPS), bn_ref[1:2, :]


def normed(z, coef):
    if coef is None:
        return z.astype(F32)
    mean, scale, shift = coef
    return jnp.maximum((z - mean) * scale + shift, 0.0)


def column_sums(z):
    z3 = z.reshape(z.shape[0] // 8, 8, z.shape[1])
    return jnp.sum(z3, axis=0), jnp.sum(z3 * z3, axis=0)


def add_sums(st_ref, z, cols):
    first, second = column_sums(z)
    st_ref[0, :, cols] += first
    st_ref[1, :, cols] += second


def greet(n):
    me = lax.axis_index("sp")
    barrier = pltpu.get_barrier_semaphore()
    for d in range(1, n):
        pl.semaphore_signal(barrier, 1, device_id={"sp": lax.rem(me + d, n)}, device_id_type=pl.DeviceIdType.MESH)
    pl.semaphore_wait(barrier, n - 1)


def exchange_sums(n, st_ref, own, slots, send_sem, recv_sem, tot_ref):
    me = lax.axis_index("sp")
    own[2:8, :] = jnp.zeros((6, own.shape[1]), F32)
    own[0:1, :] = jnp.sum(st_ref[0], axis=0, keepdims=True)
    own[1:2, :] = jnp.sum(st_ref[1], axis=0, keepdims=True)
    copies = [
        pltpu.make_async_remote_copy(
            src_ref=own,
            dst_ref=slots.at[d - 1],
            send_sem=send_sem.at[d - 1],
            recv_sem=recv_sem.at[d - 1],
            device_id={"sp": lax.rem(me + d, n)},
            device_id_type=pl.DeviceIdType.MESH,
        )
        for d in range(1, n)
    ]
    for copy in copies:
        copy.start()
    for copy in copies:
        copy.wait()
    total = own[...]
    for d in range(n - 1):
        total = total + slots[d]
    tot_ref[...] = total


def shifted(hf):
    width = hf.shape[0]
    col = lax.broadcasted_iota(jnp.int32, hf.shape, 0)
    left = jnp.where(col == 0, 0.0, pltpu.roll(hf, 1, 0)).astype(BF)
    right = jnp.where(col == width - 1, 0.0, pltpu.roll(hf, width - 1, 0)).astype(BF)
    return left, right


def split_columns(hf, lanes, slot):
    width, chans = hf.shape
    for half in range(chans // 128):
        lanes[slot, half] = hf[:, half * 128 : (half + 1) * 128]
    return [
        jnp.concatenate([lanes[slot, half, pl.ds(parity, width // 2, stride=2), :] for half in range(chans // 128)], axis=1)
        for parity in range(2)
    ]


def halo_copy(sbuf, halo, send_sem, recv_sem, way, image, peer):
    return pltpu.make_async_remote_copy(
        src_ref=sbuf.at[way, image],
        dst_ref=halo.at[way, image],
        send_sem=send_sem.at[way, image],
        recv_sem=recv_sem.at[way, image],
        device_id={"sp": peer},
        device_id_type=pl.DeviceIdType.MESH,
    )


def conv_kernel(n, images, kind, normalize, count, *refs):
    refs = list(refs)
    xa_ref, xb_ref = refs.pop(0), refs.pop(0)
    edge_refs = [refs.pop(0) for _ in range(1 if kind == "down" else 2)]
    tot_in, bn_ref = (refs.pop(0), refs.pop(0)) if normalize else (None, None)
    w_ref, z_ref, tot_ref, buf0, buf1, sbuf, halo, st, own, slots, hs_sem, hr_sem, ss_sem, sr_sem, *rest = refs
    lanes = rest[0] if rest else None
    bufs = (buf0, buf1)
    t = pl.program_id(0)
    pairs = images // 2
    me = lax.axis_index("sp")
    down = kind == "down"
    rows, width, chans = xa_ref.shape[1:]
    out_chans = z_ref.shape[3]
    ways = ((0, me > 0, me < n - 1, me + 1), (1, me < n - 1, me > 0, me - 1))
    if down:
        ways = ((0, me < n - 1, me > 0, me - 1),)

    def coef():
        return coefficients(tot_in, bn_ref, count) if normalize else None

    def start_sends(pair):
        for way, _, sends, peer in ways:
            @pl.when(sends)
            def _():
                for k in range(2):
                    halo_copy(sbuf, halo, hs_sem, hr_sem, way, 2 * pair + k, peer).start()

    def wait_halo(image):
        for way, receives, _, peer in ways:
            @pl.when(receives)
            def _():
                halo_copy(sbuf, halo, hs_sem, hr_sem, way, image, peer).wait_recv()

    def edge_rows(pair):
        c = coef()
        if down:
            for k in range(2):
                even, odd = split_columns(normed(edge_refs[0][k, 0], c), lanes, rows + k)
                sbuf[0, 2 * pair + k, 0] = even.astype(BF)
                sbuf[0, 2 * pair + k, 1] = odd.astype(BF)
            return
        sbuf[1, pl.ds(2 * pair, 2)] = normed(edge_refs[0][:, 0], None if c is None else [v[None] for v in c]).astype(BF)
        sbuf[0, pl.ds(2 * pair, 2)] = normed(edge_refs[1][:, 0], None if c is None else [v[None] for v in c]).astype(BF)

    def prep(image, x_ref, buf):
        c = coef()
        if down:
            for r in range(rows):
                even, odd = split_columns(normed(x_ref[0, r], c), lanes, r)
                buf[r, :, 0:chans] = even.astype(BF)
                buf[r, :, chans : 2 * chans] = odd.astype(BF)
                buf[r, :, 2 * chans :] = shifted(even)[1]
            even = halo[0, image, 0]
            buf[rows, :, 0:chans] = even
            buf[rows, :, chans : 2 * chans] = halo[0, image, 1]
            buf[rows, :, 2 * chans :] = shifted(even.astype(F32))[1]
            return
        for r in range(rows):
            hf = normed(x_ref[0, r], c)
            left, right = shifted(hf)
            buf[r + 1, :, 0:chans] = left
            buf[r + 1, :, chans : 2 * chans] = hf.astype(BF)
            buf[r + 1, :, 2 * chans :] = right
        for way, r in ((0, 0), (1, rows + 1)):
            h = halo[way, image]
            left, right = shifted(h.astype(F32))
            buf[r, :, 0:chans] = left
            buf[r, :, chans : 2 * chans] = h
            buf[r, :, 2 * chans :] = right

    def multiply(k, buf):
        out_rows = z_ref.shape[1]
        step = 2 if down else 1
        if kind == "a":
            for r in range(out_rows):
                lhs = jnp.concatenate([buf[r], buf[r + 1], buf[r + 2]], axis=1)
                z = jnp.dot(lhs, w_ref[...], preferred_element_type=F32)
                z_ref[k, r] = z
                add_sums(st, z, slice(0, out_chans))
            return
        lhs = jnp.concatenate(
            [jnp.concatenate([buf[step * r + dy] for r in range(out_rows)], axis=0) for dy in range(3)], axis=1
        )
        for first in range(0, out_chans, 2 * TILE):
            cols = slice(first, first + 2 * TILE)
            z = jnp.dot(lhs, w_ref[:, cols], preferred_element_type=F32)
            for r in range(out_rows):
                z_ref[k, r, :, cols] = z[r * z_ref.shape[2] : (r + 1) * z_ref.shape[2]]
            add_sums(st, z, cols)

    @pl.when(t == 0)
    def _():
        greet(n)
        st[...] = jnp.zeros_like(st)
        for way, receives, _, _ in ways:
            @pl.when(jnp.logical_not(receives))
            def _():
                halo[way] = jnp.zeros(halo.shape[1:], BF)

    @pl.when(jnp.logical_and(t >= 1, t <= pairs))
    def _():
        start_sends(t - 1)

    @pl.when(t < LEAD)
    def _():
        edge_rows(t)

    @pl.when(t == LEAD - 1)
    def _():
        wait_halo(0)
        prep(0, xb_ref, bufs[0])

    @pl.when(t >= LEAD)
    def _():
        pair = t - LEAD
        after = jnp.minimum(2 * pair + 2, images - 1)
        wait_halo(2 * pair + 1)

        @pl.when(pair < pairs - 1)
        def _():
            wait_halo(2 * pair + 2)

        multiply(0, bufs[0])
        prep(2 * pair + 1, xa_ref, bufs[1])
        multiply(1, bufs[1])
        prep(after, xb_ref, bufs[0])
        edge_rows(jnp.minimum(t, pairs))

    @pl.when(t == pairs + LEAD - 1)
    def _():
        for way, _, sends, peer in ways:
            @pl.when(sends)
            def _():
                @pl.loop(0, images)
                def _(image):
                    halo_copy(sbuf, halo, hs_sem, hr_sem, way, image, peer).wait_send()

        exchange_sums(n, st, own, slots, ss_sem, sr_sem, tot_ref)


def sum_scratch(n, chans):
    return [pltpu.VMEM((2, 8, chans), F32), pltpu.VMEM((8, chans), F32), pltpu.VMEM((n - 1, 8, chans), F32)]


def conv_layer(n, kind, collective_id, x, moments, w):
    images, rows, width, chans = x.shape
    out_chans = w.shape[-1]
    down = kind == "down"
    out_rows, out_width = (rows // 2, width // 2) if down else (rows, width)
    pairs = images // 2
    last = images - 1
    whole = lambda a: pl.BlockSpec(a.shape, lambda t: (0,) * a.ndim, pipeline_mode=pl.Buffered(1))
    edge = lambda row: pl.BlockSpec((2, 1, width, chans), lambda t: (jnp.minimum(t, pairs - 1), row, 0, 0))
    w2 = w.reshape(9 * chans, out_chans)
    in_specs = [
        pl.BlockSpec((1, rows, width, chans), lambda t: (jnp.clip(2 * (t - LEAD) + 1, 1, last), 0, 0, 0)),
        pl.BlockSpec((1, rows, width, chans), lambda t: (jnp.clip(2 * (t - LEAD) + 2, 0, last), 0, 0, 0)),
        edge(0),
    ] + ([] if down else [edge(rows - 1)])
    args = [x] * len(in_specs)
    count = 1.0
    if moments is not None:
        tot, bn = moments
        count = float(images * rows * width * n)
        in_specs += [whole(tot), whole(bn)]
        args += [tot, bn]
    in_specs.append(whole(w2))
    args.append(w2)
    n_ways = 1 if down else 2
    message = (2, width // 2, chans) if down else (width, chans)
    buf = pltpu.VMEM((rows + 1, width // 2, 3 * chans) if down else (rows + 2, width, 3 * chans), BF)
    pixels = images * out_rows * out_width
    return pl.pallas_call(
        functools.partial(conv_kernel, n, images, kind, moments is not None, count),
        grid=(pairs + LEAD,),
        in_specs=in_specs,
        out_specs=[
            pl.BlockSpec((2, out_rows, out_width, out_chans), lambda t: (jnp.maximum(t - LEAD, 0), 0, 0, 0)),
            pl.BlockSpec((8, out_chans), lambda t: (0, 0)),
        ],
        out_shape=[
            jax.ShapeDtypeStruct((images, out_rows, out_width, out_chans), F32),
            jax.ShapeDtypeStruct((8, out_chans), F32),
        ],
        scratch_shapes=[
            buf,
            buf,
            pltpu.VMEM((n_ways, images + 2) + message, BF),
            pltpu.VMEM((n_ways, images) + message, BF),
            *sum_scratch(n, out_chans),
            pltpu.SemaphoreType.DMA((n_ways, images)),
            pltpu.SemaphoreType.DMA((n_ways, images)),
            pltpu.SemaphoreType.DMA((n - 1,)),
            pltpu.SemaphoreType.DMA((n - 1,)),
        ]
        + ([pltpu.VMEM((rows + 2, chans // 128, width, 128), F32)] if down else []),
        compiler_params=pltpu.CompilerParams(collective_id=collective_id, has_side_effects=True, vmem_limit_bytes=VMEM),
        cost_estimate=pl.CostEstimate(flops=2 * pixels * 9 * chans * out_chans, bytes_accessed=x.nbytes + pixels * out_chans * 4, transcendentals=0),
        name=f"conv_{kind}",
    )(*args)


def dot_tiles(lhs_ref, w_ref, emit):
    for r in range(2):
        for first in range(0, w_ref.shape[1], 2 * TILE):
            cols = slice(first, first + 2 * TILE)
            emit(r, cols, jnp.dot(lhs_ref[0, r], w_ref[:, cols], preferred_element_type=F32))


def around(n, st, own, slots, ss_sem, sr_sem, tot_ref, images, work):
    s = pl.program_id(0)

    @pl.when(s == 0)
    def _():
        greet(n)
        st[...] = jnp.zeros_like(st)

    work()

    @pl.when(s == images - 1)
    def _():
        exchange_sums(n, st, own, slots, ss_sem, sr_sem, tot_ref)


def enter_kernel(n, images, count, x_ref, tot_in, bn_ref, w_ref, h_ref, z_ref, tot_ref, st, own, slots, ss_sem, sr_sem):
    def work():
        c = coefficients(tot_in, bn_ref, count)
        for r in range(2):
            h_ref[0, r] = normed(x_ref[0, r], c).astype(BF)

        def emit(r, cols, z):
            z_ref[0, r, :, cols] = z
            add_sums(st, z, cols)

        dot_tiles(h_ref, w_ref, emit)

    around(n, st, own, slots, ss_sem, sr_sem, tot_ref, images, work)


def sums_kernel(n, images, count, x_ref, tot_in, bn_ref, w_ref, u_ref, tot_ref, st, own, slots, ss_sem, sr_sem):
    def work():
        c = coefficients(tot_in, bn_ref, count)
        for r in range(2):
            u_ref[0, r] = normed(x_ref[0, r], c).astype(BF)
        dot_tiles(u_ref, w_ref, lambda r, cols, z: add_sums(st, z, cols))

    around(n, st, own, slots, ss_sem, sr_sem, tot_ref, images, work)


def leave(u_ref, h_ref, tot_in, bn_ref, w_ref, o_ref, count):
    mean, scale, shift = coefficients(tot_in, bn_ref, count)

    def emit(r, cols, z):
        y = (z - mean[:, cols]) * scale[:, cols] + shift[:, cols] + h_ref[0, r, :, cols].astype(F32)
        o_ref[0, r, :, cols] = jnp.maximum(y, 0.0).astype(BF)

    dot_tiles(u_ref, w_ref, emit)


def leave_enter_kernel(n, images, count, u_ref, h_ref, tot_in, bn_ref, w_ref, w_next, o_ref, z_ref, tot_ref, st, own, slots, ss_sem, sr_sem):
    def work():
        leave(u_ref, h_ref, tot_in, bn_ref, w_ref, o_ref, count)

        def emit(r, cols, z):
            z_ref[0, r, :, cols] = z
            add_sums(st, z, cols)

        dot_tiles(o_ref, w_next, emit)

    around(n, st, own, slots, ss_sem, sr_sem, tot_ref, images, work)


def leave_kernel(count, u_ref, h_ref, tot_in, bn_ref, w_ref, o_ref):
    leave(u_ref, h_ref, tot_in, bn_ref, w_ref, o_ref, count)


def point_call(n, kernel, collective_id, name, blocked, fixed, outs, sums, flops):
    images, rows, width = blocked[0].shape[:3]
    count = float(images * rows * width * n)
    block = lambda c: pl.BlockSpec((1, rows, width, c), lambda s: (s, 0, 0, 0))
    whole = lambda a: pl.BlockSpec(a.shape, lambda s: (0,) * a.ndim, pipeline_mode=pl.Buffered(1))
    out_specs = [block(c) for c, _ in outs]
    out_shape = [jax.ShapeDtypeStruct((images, rows, width, c), d) for c, d in outs]
    scratch = []
    if sums:
        out_specs.append(pl.BlockSpec((8, sums), lambda s: (0, 0)))
        out_shape.append(jax.ShapeDtypeStruct((8, sums), F32))
        scratch = [*sum_scratch(n, sums), pltpu.SemaphoreType.DMA((n - 1,)), pltpu.SemaphoreType.DMA((n - 1,))]
        kernel = functools.partial(kernel, n, images, count)
        params = pltpu.CompilerParams(collective_id=collective_id, has_side_effects=True, vmem_limit_bytes=VMEM)
    else:
        kernel = functools.partial(kernel, count)
        params = pltpu.CompilerParams(vmem_limit_bytes=VMEM)
    return pl.pallas_call(
        kernel,
        grid=(images,),
        in_specs=[block(a.shape[3]) for a in blocked] + [whole(a) for a in fixed],
        out_specs=out_specs,
        out_shape=out_shape,
        scratch_shapes=scratch,
        compiler_params=params,
        cost_estimate=pl.CostEstimate(flops=flops, bytes_accessed=sum(a.nbytes for a in blocked), transcendentals=0),
        name=name,
    )(*blocked, *fixed)


def solution(mesh):
    n = mesh.shape["sp"]

    def forward(images, w_a, bn_a, w_down, bn_down, w_in, bn_in, w_mid, bn_mid, w_out, bn_out):
        z, tot = conv_layer(n, "a", 0, images, None, w_a[0])
        for layer in range(1, w_a.shape[0]):
            z, tot = conv_layer(n, "a", 1, z, (tot, bn_a[layer - 1]), w_a[layer])
        z, tot = conv_layer(n, "down", 2, z, (tot, bn_a[w_a.shape[0] - 1]), w_down)
        wide, slim = w_down.shape[-1], w_in.shape[-1]
        pixels = z.shape[0] * z.shape[1] * z.shape[2]
        flops = 2 * pixels * wide * slim
        hidden, z, tot = point_call(n, enter_kernel, 3, "enter", [z], [tot, bn_down, w_in[0]], [(wide, BF), (slim, F32)], slim, flops)
        blocks = w_in.shape[0]
        for block in range(blocks):
            z, tot = conv_layer(n, "mid", 4, z, (tot, bn_in[block]), w_mid[block])
            branch, tot = point_call(n, sums_kernel, 5, "sums", [z], [tot, bn_mid[block], w_out[block]], [(slim, BF)], wide, flops)
            fixed = [tot, bn_out[block], w_out[block]]
            if block + 1 < blocks:
                hidden, z, tot = point_call(n, leave_enter_kernel, 6, "leave_enter", [branch, hidden], fixed + [w_in[block + 1]], [(wide, BF), (slim, F32)], slim, 2 * flops)
            else:
                hidden = point_call(n, leave_kernel, None, "leave", [branch, hidden], fixed, [(wide, BF)], 0, flops)[0]
        return hidden

    act_spec = P("dp", "sp", None, None)
    return jax.shard_map(forward, mesh=mesh, in_specs=(act_spec,) + (P(),) * 10, out_specs=act_spec, check_vma=False)
```

```python
import functools
import itertools

import jax
import jax.numpy as jnp
from jax import lax
from jax.experimental import pallas as pl
from jax.experimental.pallas import tpu as pltpu
from jax.sharding import PartitionSpec as P

NORM_EPS = 1e-5
BF, F32 = jnp.bfloat16, jnp.float32
TILE = 256
PER_STEP = {"enter": 2, "sums": 2, "leave_enter": 2, "leave": 2}
LEAD = 3
VMEM = 64000 * 1024


def coefficients(tot_ref, bn_ref, count):
    mean = tot_ref[0:1, :] / count
    var = tot_ref[1:2, :] / count - mean * mean
    return mean, bn_ref[0:1, :] * lax.rsqrt(var + NORM_EPS), bn_ref[1:2, :]


def normed(z, coef):
    if coef is None:
        return z.astype(F32)
    mean, scale, shift = coef
    return jnp.maximum((z - mean) * scale + shift, 0.0)


def column_sums(z):
    z3 = z.reshape(z.shape[0] // 8, 8, z.shape[1])
    return jnp.sum(z3, axis=0), jnp.sum(z3 * z3, axis=0)


def add_sums(st_ref, z, cols):
    first, second = column_sums(z)
    st_ref[0, :, cols] += first
    st_ref[1, :, cols] += second


def greet(n):
    me = lax.axis_index("sp")
    for d in range(1, n):
        pl.semaphore_signal(
            pltpu.get_barrier_semaphore(), 1, device_id={"sp": lax.rem(me + d, n)}, device_id_type=pl.DeviceIdType.MESH
        )


def await_greetings(n):
    pl.semaphore_wait(pltpu.get_barrier_semaphore(), n - 1)


def sum_copies(n, own, slots, send_sem, recv_sem):
    me = lax.axis_index("sp")
    return [
        pltpu.make_async_remote_copy(
            src_ref=own,
            dst_ref=slots.at[d - 1],
            send_sem=send_sem.at[d - 1],
            recv_sem=recv_sem.at[d - 1],
            device_id={"sp": lax.rem(me + d, n)},
            device_id_type=pl.DeviceIdType.MESH,
        )
        for d in range(1, n)
    ]


def send_sums(n, st_ref, own, slots, send_sem, recv_sem):
    own[0:1, :] = jnp.sum(st_ref[0], axis=0, keepdims=True)
    own[1:2, :] = jnp.sum(st_ref[1], axis=0, keepdims=True)
    for copy in sum_copies(n, own, slots, send_sem, recv_sem):
        copy.start()


def receive_sums(n, own, slots, send_sem, recv_sem, tot_ref):
    for copy in sum_copies(n, own, slots, send_sem, recv_sem):
        copy.wait()
    total = own[...]
    for d in range(n - 1):
        total = total + slots[d]
    tot_ref[...] = total


def shifted(hf):
    width = hf.shape[0]
    col = lax.broadcasted_iota(jnp.int32, hf.shape, 0)
    left = jnp.where(col == 0, 0.0, pltpu.roll(hf, 1, 0)).astype(BF)
    right = jnp.where(col == width - 1, 0.0, pltpu.roll(hf, width - 1, 0)).astype(BF)
    return left, right


def split_columns(hf, lanes, slot):
    width, chans = hf.shape
    for half in range(chans // 128):
        lanes[slot, half] = hf[:, half * 128 : (half + 1) * 128]
    return [
        jnp.concatenate([lanes[slot, half, pl.ds(parity, width // 2, stride=2), :] for half in range(chans // 128)], axis=1)
        for parity in range(2)
    ]


def halo_copy(sbuf, halo, send_sem, recv_sem, way, image, peer):
    return pltpu.make_async_remote_copy(
        src_ref=sbuf.at[way, image],
        dst_ref=halo.at[way, image],
        send_sem=send_sem.at[way, image],
        recv_sem=recv_sem.at[way, image],
        device_id={"sp": peer},
        device_id_type=pl.DeviceIdType.MESH,
    )


def conv_kernel(n, images, kind, layer, normalize, count, *refs):
    refs = list(refs)
    xa_ref, xb_ref = refs.pop(0), refs.pop(0)
    edge_refs = [refs.pop(0) for _ in range(1 if kind == "down" else 2)]
    tot_in, bn_ref = (refs.pop(0), refs.pop(0)) if normalize else (None, None)
    w_hbm, z_ref, tot_ref, w_ref, w_sem, buf0, buf1, sbuf, halo, st, own, slots, hs_sem, hr_sem, ss_sem, sr_sem, *rest = refs
    lanes = rest[0] if rest else None
    bufs = (buf0, buf1)
    t = pl.program_id(0)
    pairs = images // 2
    me = lax.axis_index("sp")
    down = kind == "down"
    rows, width, chans = xa_ref.shape[1:]
    out_chans = z_ref.shape[3]
    ways = ((0, me > 0, me < n - 1, me + 1), (1, me < n - 1, me > 0, me - 1))
    if down:
        ways = ((0, me < n - 1, me > 0, me - 1),)

    def coef():
        return coefficients(tot_in, bn_ref, count) if normalize else None

    def start_sends(pair):
        for way, _, sends, peer in ways:
            @pl.when(sends)
            def _():
                for k in range(2):
                    halo_copy(sbuf, halo, hs_sem, hr_sem, way, 2 * pair + k, peer).start()

    def wait_halo(image):
        for way, receives, _, peer in ways:
            @pl.when(receives)
            def _():
                halo_copy(sbuf, halo, hs_sem, hr_sem, way, image, peer).wait_recv()

    def edge_rows(pair):
        c = coef()
        if down:
            for k in range(2):
                even, odd = split_columns(normed(edge_refs[0][k, 0], c), lanes, rows + k)
                sbuf[0, 2 * pair + k, 0] = even.astype(BF)
                sbuf[0, 2 * pair + k, 1] = odd.astype(BF)
            return
        sbuf[1, pl.ds(2 * pair, 2)] = normed(edge_refs[0][:, 0], None if c is None else [v[None] for v in c]).astype(BF)
        sbuf[0, pl.ds(2 * pair, 2)] = normed(edge_refs[1][:, 0], None if c is None else [v[None] for v in c]).astype(BF)

    def prep_own(x_ref, buf):
        c = coef()
        if down:
            for r in range(rows):
                even, odd = split_columns(normed(x_ref[0, r], c), lanes, r)
                buf[r, :, 0:chans] = even.astype(BF)
                buf[r, :, chans : 2 * chans] = odd.astype(BF)
                buf[r, :, 2 * chans :] = shifted(even)[1]
            return
        for r in range(rows):
            hf = normed(x_ref[0, r], c)
            left, right = shifted(hf)
            buf[r + 1, :, 0:chans] = left
            buf[r + 1, :, chans : 2 * chans] = hf.astype(BF)
            buf[r + 1, :, 2 * chans :] = right

    def prep_halo(image, buf):
        if down:
            even = halo[0, image, 0]
            buf[rows, :, 0:chans] = even
            buf[rows, :, chans : 2 * chans] = halo[0, image, 1]
            buf[rows, :, 2 * chans :] = shifted(even.astype(F32))[1]
            return
        for way, r in ((0, 0), (1, rows + 1)):
            h = halo[way, image]
            left, right = shifted(h.astype(F32))
            buf[r, :, 0:chans] = left
            buf[r, :, chans : 2 * chans] = h
            buf[r, :, 2 * chans :] = right

    def multiply(k, buf):
        out_rows = z_ref.shape[1]
        if kind == "a":
            for r in range(out_rows):
                lhs = jnp.concatenate([buf[r], buf[r + 1], buf[r + 2]], axis=1)
                z = jnp.dot(lhs, w_ref[...], preferred_element_type=F32)
                z_ref[k, r] = z
                add_sums(st, z, slice(0, out_chans))
            return
        step = 2 if down else 1
        lhs = jnp.concatenate(
            [jnp.concatenate([buf[step * r + dy] for r in range(out_rows)], axis=0) for dy in range(3)], axis=1
        )
        for first in range(0, out_chans, 2 * TILE):
            cols = slice(first, first + 2 * TILE)
            z = jnp.dot(lhs, w_ref[:, cols], preferred_element_type=F32)
            for r in range(out_rows):
                z_ref[k, r, :, cols] = z[r * z_ref.shape[2] : (r + 1) * z_ref.shape[2]]
            add_sums(st, z, cols)

    load_weights = pltpu.make_async_copy(w_hbm.at[layer], w_ref, w_sem)

    @pl.when(t == 0)
    def _():
        load_weights.start()
        greet(n)
        st[...] = jnp.zeros_like(st)
        edge_rows(0)
        await_greetings(n)
        start_sends(0)

    @pl.when(jnp.logical_and(t >= 2, t <= pairs))
    def _():
        start_sends(t - 1)

    @pl.when(t == 1)
    def _():
        for way, receives, _, _ in ways:
            @pl.when(jnp.logical_not(receives))
            def _():
                halo[way] = jnp.zeros(halo.shape[1:], BF)

    @pl.when(jnp.logical_and(t >= 1, t < LEAD))
    def _():
        edge_rows(t)

    @pl.when(t == LEAD - 1)
    def _():
        prep_own(xb_ref, bufs[0])
        load_weights.wait()

    @pl.when(t >= LEAD)
    def _():
        pair = t - LEAD
        wait_halo(2 * pair)
        wait_halo(2 * pair + 1)
        prep_halo(2 * pair, bufs[0])
        multiply(0, bufs[0])
        prep_own(xa_ref, bufs[1])
        prep_halo(2 * pair + 1, bufs[1])
        multiply(1, bufs[1])
        prep_own(xb_ref, bufs[0])
        edge_rows(jnp.minimum(t, pairs))

    @pl.when(t == pairs + LEAD - 1)
    def _():
        send_sums(n, st, own, slots, ss_sem, sr_sem)
        for way, _, sends, peer in ways:
            @pl.when(sends)
            def _():
                @pl.loop(0, images)
                def _(image):
                    halo_copy(sbuf, halo, hs_sem, hr_sem, way, image, peer).wait_send()

        receive_sums(n, own, slots, ss_sem, sr_sem, tot_ref)


def sum_scratch(n, chans):
    return [pltpu.VMEM((2, 8, chans), F32), pltpu.VMEM((2, chans), F32), pltpu.VMEM((n - 1, 2, chans), F32)]


def layer_spec(stacked):
    array, layer = stacked
    return pl.BlockSpec((None,) + array.shape[1:], lambda *_: (layer, 0, 0), pipeline_mode=pl.Buffered(1))


def conv_layer(n, kind, layer, collective_id, x, moments, w):
    images, rows, width, chans = x.shape
    out_chans = w.shape[-1]
    down = kind == "down"
    out_rows, out_width = (rows // 2, width // 2) if down else (rows, width)
    pairs = images // 2
    last = images - 1
    whole = lambda a: pl.BlockSpec(a.shape, lambda t: (0,) * a.ndim, pipeline_mode=pl.Buffered(1))
    edge = lambda row: pl.BlockSpec((2, 1, width, chans), lambda t: (jnp.minimum(t, pairs - 1), row, 0, 0))
    w2 = w.reshape(-1, 9 * chans, out_chans)
    in_specs = [
        pl.BlockSpec((1, rows, width, chans), lambda t: (jnp.clip(2 * (t - LEAD) + 1, 1, last), 0, 0, 0)),
        pl.BlockSpec((1, rows, width, chans), lambda t: (jnp.clip(2 * (t - LEAD) + 2, 0, last), 0, 0, 0)),
        edge(0),
    ] + ([] if down else [edge(rows - 1)])
    args = [x] * len(in_specs)
    count = 1.0
    if moments is not None:
        tot, bn = moments
        count = float(images * rows * width * n)
        in_specs += [whole(tot), layer_spec(bn)]
        args += [tot, bn[0]]
    in_specs.append(pl.BlockSpec(memory_space=pl.ANY))
    args.append(w2)
    n_ways = 1 if down else 2
    message = (2, width // 2, chans) if down else (width, chans)
    buf = pltpu.VMEM((rows + 1, width // 2, 3 * chans) if down else (rows + 2, width, 3 * chans), BF)
    pixels = images * out_rows * out_width
    return pl.pallas_call(
        functools.partial(conv_kernel, n, images, kind, layer, moments is not None, count),
        grid=(pairs + LEAD,),
        in_specs=in_specs,
        out_specs=[
            pl.BlockSpec((2, out_rows, out_width, out_chans), lambda t: (jnp.maximum(t - LEAD, 0), 0, 0, 0)),
            pl.BlockSpec((2, out_chans), lambda t: (0, 0)),
        ],
        out_shape=[
            jax.ShapeDtypeStruct((images, out_rows, out_width, out_chans), F32),
            jax.ShapeDtypeStruct((2, out_chans), F32),
        ],
        scratch_shapes=[
            pltpu.VMEM(w2.shape[1:], BF),
            pltpu.SemaphoreType.DMA,
            buf,
            buf,
            pltpu.VMEM((n_ways, images + 2) + message, BF),
            pltpu.VMEM((n_ways, images) + message, BF),
            *sum_scratch(n, out_chans),
            pltpu.SemaphoreType.DMA((n_ways, images)),
            pltpu.SemaphoreType.DMA((n_ways, images)),
            pltpu.SemaphoreType.DMA((n - 1,)),
            pltpu.SemaphoreType.DMA((n - 1,)),
        ]
        + ([pltpu.VMEM((rows + 2, chans // 128, width, 128), F32)] if down else []),
        compiler_params=pltpu.CompilerParams(collective_id=collective_id, has_side_effects=True, vmem_limit_bytes=VMEM),
        cost_estimate=pl.CostEstimate(flops=2 * pixels * 9 * chans * out_chans, bytes_accessed=x.nbytes + pixels * out_chans * 4, transcendentals=0),
        name=f"conv_{kind}",
    )(*args)


def dot_tiles(lhs_ref, w_ref, emit):
    lhs = lhs_ref[...].reshape(-1, lhs_ref.shape[3])
    for first in range(0, w_ref.shape[1], 2 * TILE):
        cols = slice(first, first + 2 * TILE)
        emit(cols, jnp.dot(lhs, w_ref[:, cols], preferred_element_type=F32))


def around(n, st, own, slots, ss_sem, sr_sem, tot_ref, work):
    s = pl.program_id(0)

    @pl.when(s == 0)
    def _():
        greet(n)
        st[...] = jnp.zeros_like(st)

    work()

    @pl.when(s == pl.num_programs(0) - 1)
    def _():
        await_greetings(n)
        send_sums(n, st, own, slots, ss_sem, sr_sem)
        receive_sums(n, own, slots, ss_sem, sr_sem, tot_ref)


def enter_kernel(n, count, x_ref, tot_in, bn_ref, w_ref, h_ref, z_ref, tot_ref, st, own, slots, ss_sem, sr_sem):
    def work():
        c = coefficients(tot_in, bn_ref, count)
        for k in range(x_ref.shape[0]):
            for r in range(x_ref.shape[1]):
                h_ref[k, r] = normed(x_ref[k, r], c).astype(BF)

        def emit(cols, z):
            z_ref[:, :, :, cols] = z.reshape(z_ref.shape[:3] + z.shape[1:])
            add_sums(st, z, cols)

        dot_tiles(h_ref, w_ref, emit)

    around(n, st, own, slots, ss_sem, sr_sem, tot_ref, work)


def sums_kernel(n, count, x_ref, tot_in, bn_ref, w_ref, u_ref, tot_ref, st, own, slots, ss_sem, sr_sem):
    def work():
        c = coefficients(tot_in, bn_ref, count)
        for k in range(x_ref.shape[0]):
            for r in range(x_ref.shape[1]):
                u_ref[k, r] = normed(x_ref[k, r], c).astype(BF)
        dot_tiles(u_ref, w_ref, lambda cols, z: add_sums(st, z, cols))

    around(n, st, own, slots, ss_sem, sr_sem, tot_ref, work)


def leave(u_ref, h_ref, tot_in, bn_ref, w_ref, o_ref, count):
    mean, scale, shift = coefficients(tot_in, bn_ref, count)

    def emit(cols, z):
        y = (z - mean[:, cols]) * scale[:, cols] + shift[:, cols]
        y = y + h_ref[:, :, :, cols].astype(F32).reshape(y.shape)
        o_ref[:, :, :, cols] = jnp.maximum(y, 0.0).astype(BF).reshape(o_ref.shape[:3] + y.shape[1:])

    dot_tiles(u_ref, w_ref, emit)


def leave_enter_kernel(n, count, u_ref, h_ref, tot_in, bn_ref, w_ref, w_next, o_ref, z_ref, tot_ref, st, own, slots, ss_sem, sr_sem):
    def work():
        leave(u_ref, h_ref, tot_in, bn_ref, w_ref, o_ref, count)

        def emit(cols, z):
            z_ref[:, :, :, cols] = z.reshape(z_ref.shape[:3] + z.shape[1:])
            add_sums(st, z, cols)

        dot_tiles(o_ref, w_next, emit)

    around(n, st, own, slots, ss_sem, sr_sem, tot_ref, work)


def leave_kernel(count, u_ref, h_ref, tot_in, bn_ref, w_ref, o_ref):
    leave(u_ref, h_ref, tot_in, bn_ref, w_ref, o_ref, count)


def point_call(n, kernel, collective_id, name, per_step, blocked, fixed, outs, sums, flops):
    images, rows, width = blocked[0].shape[:3]
    count = float(images * rows * width * n)
    block = lambda c: pl.BlockSpec((per_step, rows, width, c), lambda s: (s, 0, 0, 0))
    whole = lambda a: pl.BlockSpec(a.shape, lambda s: (0,) * a.ndim, pipeline_mode=pl.Buffered(1))
    out_specs = [block(c) for c, _ in outs]
    out_shape = [jax.ShapeDtypeStruct((images, rows, width, c), d) for c, d in outs]
    scratch = []
    if sums:
        out_specs.append(pl.BlockSpec((2, sums), lambda s: (0, 0)))
        out_shape.append(jax.ShapeDtypeStruct((2, sums), F32))
        scratch = [*sum_scratch(n, sums), pltpu.SemaphoreType.DMA((n - 1,)), pltpu.SemaphoreType.DMA((n - 1,))]
        kernel = functools.partial(kernel, n, count)
        params = pltpu.CompilerParams(collective_id=collective_id, has_side_effects=True, vmem_limit_bytes=VMEM)
    else:
        kernel = functools.partial(kernel, count)
        params = pltpu.CompilerParams(vmem_limit_bytes=VMEM)
    return pl.pallas_call(
        kernel,
        grid=(images // per_step,),
        in_specs=[block(a.shape[3]) for a in blocked] + [layer_spec(a) if isinstance(a, tuple) else whole(a) for a in fixed],
        out_specs=out_specs,
        out_shape=out_shape,
        scratch_shapes=scratch,
        compiler_params=params,
        cost_estimate=pl.CostEstimate(flops=flops, bytes_accessed=sum(a.nbytes for a in blocked), transcendentals=0),
        name=name,
    )(*blocked, *[a[0] if isinstance(a, tuple) else a for a in fixed])


def solution(mesh):
    n = mesh.shape["sp"]

    def forward(images, w_a, bn_a, w_down, bn_down, w_in, bn_in, w_mid, bn_mid, w_out, bn_out):
        layers, blocks = w_a.shape[0], w_in.shape[0]
        ids = itertools.count()
        bn_down = bn_down[None]
        z, tot = conv_layer(n, "a", 0, next(ids), images, None, w_a)
        for layer in range(1, layers):
            z, tot = conv_layer(n, "a", layer, next(ids), z, (tot, (bn_a, layer - 1)), w_a)
        z, tot = conv_layer(n, "down", 0, next(ids), z, (tot, (bn_a, layers - 1)), w_down)
        wide, slim = w_down.shape[-1], w_in.shape[-1]
        pixels = z.shape[0] * z.shape[1] * z.shape[2]
        flops = 2 * pixels * wide * slim
        hidden, z, tot = point_call(n, enter_kernel, next(ids), "enter", PER_STEP["enter"], [z], [tot, (bn_down, 0), (w_in, 0)], [(wide, BF), (slim, F32)], slim, flops)
        for block in range(blocks):
            z, tot = conv_layer(n, "mid", block, next(ids), z, (tot, (bn_in, block)), w_mid)
            branch, tot = point_call(n, sums_kernel, next(ids), "sums", PER_STEP["sums"], [z], [tot, (bn_mid, block), (w_out, block)], [(slim, BF)], wide, flops)
            fixed = [tot, (bn_out, block), (w_out, block)]
            if block + 1 < blocks:
                hidden, z, tot = point_call(n, leave_enter_kernel, next(ids), "leave_enter", PER_STEP["leave_enter"], [branch, hidden], fixed + [(w_in, block + 1)], [(wide, BF), (slim, F32)], slim, 2 * flops)
            else:
                hidden = point_call(n, leave_kernel, None, "leave", PER_STEP["leave"], [branch, hidden], fixed, [(wide, BF)], 0, flops)[0]
        return hidden

    act_spec = P("dp", "sp", None, None)
    return jax.shard_map(forward, mesh=mesh, in_specs=(act_spec,) + (P(),) * 10, out_specs=act_spec, check_vma=False)
```
